8 devices in a mesh: dp: 1 (over z), tp: 2 (over y), cp: 4 (over x, core).
Axes of the slice: x: 2, y: 2, z: 1, core: 2. Of those that a mesh axis runs over, the one named last changes fastest.
Arguments:
- hidden: bfloat16 [8192, 2304], P(('dp', 'cp'))
- positions: int32 [8192], P(('dp', 'cp'))
- w_q: bfloat16 [2, 2304, 2048], P(None, None, 'tp')
- w_k: bfloat16 [2, 2304, 1024], P(None, None, 'tp')
- w_v: bfloat16 [2, 2304, 1024], P(None, None, 'tp')
- w_o: bfloat16 [2, 2048, 2304], P(None, 'tp')
- w_gate: bfloat16 [2, 2304, 9216], P(None, None, 'tp')
- w_up: bfloat16 [2, 2304, 9216], P(None, None, 'tp')
- w_down: bfloat16 [2, 9216, 2304], P(None, 'tp')
- norm_gain: float32 [2, 4, 2304], replicated
- qk_gain: float32 [2, 2, 256], replicated
Outputs:
- output 1: bfloat16 [8192, 2304], P(('dp', 'cp'))
- output 2: bfloat16 [2, 8192, 4, 256], P(None, ('dp', 'cp'), 'tp')
- output 3: bfloat16 [2, 8192, 4, 256], P(None, ('dp', 'cp'), 'tp')
All inputs are finite; a program needn't handle non-finite values.
Results may differ from the reference program's by a relative error of at most 0.0163912.
Values are sent between devices in bfloat16 or wider.
A program may use at most 1 GiB of HBM per device.

```python
import jax
import jax.numpy as jnp
from jax import lax

D = 2304
HEADS = 8
KV_HEADS = 4
HEAD = 256
FF = 9216
WINDOW = 1024
TOKENS = 8192

EPS = 1e-6
THETAS = (10000.0, 1000000.0)
LAYER_WINDOWS = (WINDOW, TOKENS)
Q_BLOCK = min(32, TOKENS)


def normal_weight(key_in, arr_shape, fan_in):
    scale_val = fan_in ** -0.5
    return (jax.random.normal(key_in, arr_shape, jnp.float32) * scale_val).astype(jnp.bfloat16)


def setup_inputs(seed: int = 0, part: int = 0) -> dict:
    part_key = jax.random.fold_in(jax.random.key(seed), part)
    key_hidden, key_start = jax.random.split(part_key, 2)
    shared = jax.random.split(jax.random.key(seed + 1), 9)
    hidden = jax.random.normal(key_hidden, (TOKENS, D), jnp.float32).astype(jnp.bfloat16)
    start_pos = jax.random.randint(key_start, (), 0, 1024)
    positions = (start_pos + jnp.arange(TOKENS)).astype(jnp.int32)
    return {
        'hidden': hidden,
        'positions': positions,
        'w_q': normal_weight(shared[0], (2, D, HEADS * HEAD), D),
        'w_k': normal_weight(shared[1], (2, D, KV_HEADS * HEAD), D),
        'w_v': normal_weight(shared[2], (2, D, KV_HEADS * HEAD), D),
        'w_o': normal_weight(shared[3], (2, HEADS * HEAD, D), HEADS * HEAD),
        'w_gate': normal_weight(shared[4], (2, D, FF), D),
        'w_up': normal_weight(shared[5], (2, D, FF), D),
        'w_down': normal_weight(shared[6], (2, FF, D), FF),
        'norm_gain': 0.4 * jax.random.normal(shared[7], (2, 4, D), jnp.float32),
        'qk_gain': 0.4 * jax.random.normal(shared[8], (2, 2, HEAD), jnp.float32),
    }


def rms_scale(values, gain):
    mean_sq = jnp.mean(values * values, axis=-1, keepdims=True)
    return values * lax.rsqrt(mean_sq + EPS) * (1.0 + gain)


def rotary(values, positions, theta):
    half_dim = HEAD // 2
    inv_freq = theta ** (-(jnp.arange(half_dim, dtype=jnp.float32) * 2.0) / HEAD)
    angles = positions.astype(jnp.float32)[..., None] * inv_freq
    cosine = jnp.cos(angles)[..., None, :]
    sine_val = jnp.sin(angles)[..., None, :]
    lower_half = values[..., :half_dim]
    upper_half = values[..., half_dim:]
    return jnp.concatenate([lower_half * cosine - upper_half * sine_val, upper_half * cosine + lower_half * sine_val], axis=-1)


def attention(queries, key_rows, val_rows, window):
    groups = HEADS // KV_HEADS
    score_scale = HEAD ** -0.5
    key_f = key_rows.astype(jnp.float32)
    val_f = val_rows.astype(jnp.float32)
    q_blocks = queries.reshape(TOKENS // Q_BLOCK, Q_BLOCK, KV_HEADS, groups, HEAD)
    key_index = jnp.arange(TOKENS)

    def one_block(block_args):
        q_block, block_id = block_args
        scores = jnp.einsum('qhgd,uhd->hgqu', q_block.astype(jnp.float32), key_f) * score_scale
        query_index = block_id * Q_BLOCK + jnp.arange(Q_BLOCK)
        distance = query_index[:, None] - key_index[None, :]
        allowed = (distance >= 0) & (distance < window)
        scores = jnp.where(allowed, scores, -jnp.inf)
        prob_all = jax.nn.softmax(scores, axis=-1)
        return jnp.einsum('hgqu,uhd->qhgd', prob_all, val_f)

    block_out = lax.map(one_block, (q_blocks, jnp.arange(TOKENS // Q_BLOCK)))
    return block_out.reshape(TOKENS, HEADS * HEAD).astype(jnp.bfloat16)


def reference(hidden, positions, w_q, w_k, w_v, w_o, w_gate, w_up, w_down, norm_gain, qk_gain):
    state_f = hidden.astype(jnp.float32)
    new_hidden = hidden
    k_list = []
    v_list = []
    for layer_id in range(2):
        layer_gain = norm_gain[layer_id]
        normed = rms_scale(state_f, layer_gain[0]).astype(jnp.bfloat16)
        q_proj = jnp.dot(normed, w_q[layer_id], preferred_element_type=jnp.float32).reshape(TOKENS, HEADS, HEAD)
        k_proj = jnp.dot(normed, w_k[layer_id], preferred_element_type=jnp.float32).reshape(TOKENS, KV_HEADS, HEAD)
        v_rows = jnp.dot(normed, w_v[layer_id], preferred_element_type=jnp.float32).astype(jnp.bfloat16).reshape(TOKENS, KV_HEADS, HEAD)
        q_rot = rotary(rms_scale(q_proj, qk_gain[layer_id, 0]), positions, THETAS[layer_id]).astype(jnp.bfloat16)
        k_rot = rotary(rms_scale(k_proj, qk_gain[layer_id, 1]), positions, THETAS[layer_id]).astype(jnp.bfloat16)
        attn_rows = attention(q_rot, k_rot, v_rows, LAYER_WINDOWS[layer_id])
        attn_out = jnp.dot(attn_rows, w_o[layer_id], preferred_element_type=jnp.float32)
        resid_f = (state_f + rms_scale(attn_out, layer_gain[1])).astype(jnp.bfloat16).astype(jnp.float32)
        normed_mlp = rms_scale(resid_f, layer_gain[2]).astype(jnp.bfloat16)
        gate_proj = jnp.dot(normed_mlp, w_gate[layer_id], preferred_element_type=jnp.float32)
        up_proj = jnp.dot(normed_mlp, w_up[layer_id], preferred_element_type=jnp.float32)
        act_rows = (jax.nn.gelu(gate_proj, approximate=True) * up_proj).astype(jnp.bfloat16)
        mlp_out = jnp.dot(act_rows, w_down[layer_id], preferred_element_type=jnp.float32)
        new_hidden = (resid_f + rms_scale(mlp_out, layer_gain[3])).astype(jnp.bfloat16)
        state_f = new_hidden.astype(jnp.float32)
        k_list.append(k_rot)
        v_list.append(v_rows)
    return new_hidden, jnp.stack(k_list), jnp.stack(v_list)
```

```python
import functools

import jax
import jax.numpy as jnp
from jax import lax
from jax.experimental import pallas as pl
from jax.experimental.pallas import tpu as pltpu
from jax.sharding import PartitionSpec as P


THETAS = (10000.0, 1000000.0)
EPS = 1e-6
NEG_BIG = -1e30
LOG2E = 1.4426950408889634
F32 = jnp.float32
BF16 = jnp.bfloat16
VMEM_LIMIT = 67043328
ANY = pl.BlockSpec(memory_space=pl.ANY)


def rms_scale(values, gain):
    mean_sq = jnp.mean(values * values, axis=-1, keepdims=True)
    return values * lax.rsqrt(mean_sq + EPS) * (1.0 + gain)


def once(shape, index_map):
    return pl.BlockSpec(shape, index_map, pipeline_mode=pl.Buffered(1))


def run_kernel(kernel, args, in_specs, out_shape, out_specs, grid, scalars=(), deps=(), scratch=(), flops=0, nbytes=0, aliases=None):
    n_scalar = len(scalars)
    n_in = len(args)
    n_dep = len(deps)

    def body(*refs):
        head = refs[: n_scalar + n_in]
        tail = refs[n_scalar + n_in + n_dep:]
        kernel(*head, *tail)

    return pl.pallas_call(
        body,
        out_shape=out_shape,
        grid_spec=pltpu.PrefetchScalarGridSpec(
            num_scalar_prefetch=n_scalar,
            grid=grid,
            in_specs=list(in_specs) + [ANY] * n_dep,
            out_specs=out_specs,
            scratch_shapes=list(scratch),
        ),
        compiler_params=pltpu.CompilerParams(vmem_limit_bytes=VMEM_LIMIT, dimension_semantics=("arbitrary",) * len(grid)),
        cost_estimate=pl.CostEstimate(flops=int(flops), bytes_accessed=int(nbytes), transcendentals=0),
        input_output_aliases=aliases or {},
    )(*scalars, *args, *deps)


def sds(shape, dtype):
    return jax.ShapeDtypeStruct(shape, dtype)


def project_rows(x_rows, w_q, w_k, w_v, gain, qk_gain, base_tab, off_tab, q_out, kv_out, row0, head_dim):
    normed = rms_scale(x_rows.astype(F32), gain).astype(BF16)
    rows = x_rows.shape[0]
    half = head_dim // 2
    cos_off, sin_off = off_tab[0], off_tab[1]
    cosines, sines = [], []
    for g in range(rows // 32):
        cos_base, sin_base = base_tab[0, g:g + 1, :], base_tab[1, g:g + 1, :]
        cosines.append(cos_base * cos_off - sin_base * sin_off)
        sines.append(sin_base * cos_off + cos_base * sin_off)
    cosine = jnp.concatenate(cosines, axis=0)
    sine_val = jnp.concatenate(sines, axis=0)

    def rotate(proj, head_gain):
        normed_head = rms_scale(proj, head_gain)
        lower, upper = normed_head[:, :half], normed_head[:, half:]
        return jnp.concatenate([lower * cosine - upper * sine_val, upper * cosine + lower * sine_val], axis=1).astype(BF16)

    n_kv = w_k.shape[-1] // head_dim
    for h in range(w_q.shape[-1] // head_dim):
        cols = slice(h * head_dim, (h + 1) * head_dim)
        proj = jnp.dot(normed, w_q[:, cols], preferred_element_type=F32)
        q_out[row0:row0 + rows, cols] = rotate(proj, qk_gain[0:1, :])
    for h in range(n_kv):
        cols = slice(h * head_dim, (h + 1) * head_dim)
        proj = jnp.dot(normed, w_k[:, cols], preferred_element_type=F32)
        kv_out[row0:row0 + rows, cols] = rotate(proj, qk_gain[1:2, :])
    for h in range(n_kv):
        cols = slice(h * head_dim, (h + 1) * head_dim)
        out_cols = slice((n_kv + h) * head_dim, (n_kv + h + 1) * head_dim)
        kv_out[row0:row0 + rows, out_cols] = jnp.dot(normed, w_v[:, cols], preferred_element_type=F32).astype(BF16)


def weight_specs(layer, w_q, w_k, w_v, norm_gain, qk_gain):
    return [
        once((None,) + w_q.shape[1:], lambda i, *s: (layer, 0, 0)),
        once((None,) + w_k.shape[1:], lambda i, *s: (layer, 0, 0)),
        once((None,) + w_v.shape[1:], lambda i, *s: (layer, 0, 0)),
        once((None,) + norm_gain.shape[1:], lambda i, *s: (layer, 0, 0)),
        once((None,) + qk_gain.shape[1:], lambda i, *s: (layer, 0, 0)),
    ]


def qkv_from_rows(layer, x, row0, rows, weights, tabs, deps):
    w_q, w_k, _, _, qk_gain = weights
    base_tab, off_tab = tabs
    head_dim = qk_gain.shape[-1]
    width = x.shape[1]
    bm = 256
    b0 = row0 // bm

    def kernel(x_ref, wq, wk, wv, ng, qg, bt, ot, q_out, kv_out):
        project_rows(x_ref[...], wq, wk, wv, ng[0:1, :], qg, bt, ot, q_out, kv_out, 0, head_dim)

    nq, nkv = w_q.shape[-1], 2 * w_k.shape[-1]
    return run_kernel(
        kernel, (x, *weights, base_tab, off_tab),
        [pl.BlockSpec((bm, width), lambda i: (b0 + i, 0))] + weight_specs(layer, *weights)
        + [pl.BlockSpec((None, 2, bm // 32, head_dim // 2), lambda i: (layer, 0, b0 + i, 0)),
           once((None, 2, 32, head_dim // 2), lambda i: (layer, 0, 0, 0))],
        (sds((rows, nq), BF16), sds((rows, nkv), BF16)),
        [pl.BlockSpec((bm, nq), lambda i: (i, 0)), pl.BlockSpec((bm, nkv), lambda i: (i, 0))],
        (rows // bm,), deps=deps,
        flops=2 * rows * width * (nq + nkv), nbytes=2 * width * (nq + nkv + rows),
    )


def qkv_from_pieces(layer, tp_id, x_keep, x_other, row0, weights, tabs, deps):
    w_q, w_k, _, _, qk_gain = weights
    base_tab, off_tab = tabs
    head_dim = qk_gain.shape[-1]
    bm, width = x_keep.shape
    b0 = row0 // bm

    def kernel(tp, keep_ref, other_ref, wq, wk, wv, ng, qg, bt, ot, q_out, kv_out, x_out):
        rows = jnp.where(pl.program_id(0) == 0, keep_ref[...], other_ref[...])
        x_out[...] = rows
        project_rows(rows, wq, wk, wv, ng[0:1, :], qg, bt, ot, q_out, kv_out, 0, head_dim)

    def half(i, tp):
        return lax.rem(i + tp[0], 2)

    nq, nkv = w_q.shape[-1], 2 * w_k.shape[-1]
    rows = 2 * bm
    return run_kernel(
        kernel, (x_keep, x_other, *weights, base_tab, off_tab),
        [once((bm, width), lambda i, tp: (0, 0)), once((bm, width), lambda i, tp: (0, 0))] + weight_specs(layer, *weights)
        + [pl.BlockSpec((None, 2, bm // 32, head_dim // 2), lambda i, tp: (layer, 0, b0 + half(i, tp), 0)),
           once((None, 2, 32, head_dim // 2), lambda i, tp: (layer, 0, 0, 0))],
        (sds((rows, nq), BF16), sds((rows, nkv), BF16), sds((rows, width), BF16)),
        [pl.BlockSpec((bm, nq), lambda i, tp: (half(i, tp), 0)), pl.BlockSpec((bm, nkv), lambda i, tp: (half(i, tp), 0)),
         pl.BlockSpec((bm, width), lambda i, tp: (half(i, tp), 0))],
        (2,), scalars=(tp_id,), deps=deps,
        flops=2 * rows * width * (nq + nkv), nbytes=2 * width * (nq + nkv + 2 * rows),
    )


def dot_t(a, b):
    return lax.dot_general(a, b, (((1,), (1,)), ((), ())), preferred_element_type=F32)


def local_attention(first, q, q_block, kv_blocks, head_dim, chunk, deps):
    nq = q.shape[1]
    nkv_heads = kv_blocks[0][0].shape[1] // (2 * head_dim)
    groups = nq // head_dim // nkv_heads
    factor = head_dim ** -0.5 * LOG2E
    sub = 256

    def kernel(first_ref, q_ref, ka, va, kb, vb, kc, vc, o_ref):
        key_refs, val_refs = (ka, kb, kc), (va, vb, vc)
        for g in range(groups):
            for r in range(chunk // sub):
                q_rows = q_ref[r * sub:(r + 1) * sub, g * head_dim:(g + 1) * head_dim]
                row = lax.broadcasted_iota(jnp.int32, (sub, chunk), 0) + r * sub
                col = lax.broadcasted_iota(jnp.int32, (sub, chunk), 1)
                scores = []
                for b in range(3):
                    s = dot_t(q_rows, key_refs[b][...])
                    if b == 0:
                        s = jnp.where(col > row, s, NEG_BIG)
                    if b == 2:
                        s = jnp.where(col <= row, s, NEG_BIG)
                    if kv_blocks[b][2]:
                        s = jnp.where(first_ref[0] == 1, NEG_BIG, s)
                    scores.append(s)
                top = functools.reduce(jnp.maximum, [jnp.max(s, axis=1, keepdims=True) for s in scores])
                total = jnp.zeros((sub, 1), F32)
                out = jnp.zeros((sub, head_dim), F32)
                for b in range(3):
                    p = jnp.exp2((scores[b] - top) * factor)
                    total = total + jnp.sum(p, axis=1, keepdims=True)
                    out = out + jnp.dot(p.astype(BF16), val_refs[b][...], preferred_element_type=F32)
                o_ref[r * sub:(r + 1) * sub, g * head_dim:(g + 1) * head_dim] = (out / total).astype(BF16)

    specs = [pl.BlockSpec((chunk, groups * head_dim), lambda i, f: (q_block, i))]
    args = [q]
    for array, block, _ in kv_blocks:
        specs.append(pl.BlockSpec((chunk, head_dim), lambda i, f, block=block: (block, i)))
        specs.append(pl.BlockSpec((chunk, head_dim), lambda i, f, block=block: (block, nkv_heads + i)))
        args += [array, array]
    return run_kernel(
        kernel, args, specs, sds((chunk, nq), BF16),
        pl.BlockSpec((chunk, groups * head_dim), lambda i, f: (0, i)), (nkv_heads,),
        scalars=(first,), deps=deps, flops=4 * chunk * 3 * chunk * nq, nbytes=10 * chunk * nq,
    )


def global_attention(rank, q, gathered, n_own, head_dim, chunk, deps):
    nq = q.shape[1]
    nkv_heads = gathered[0].shape[1] // (2 * head_dim)
    groups = nq // head_dim // nkv_heads
    n_chunk = len(gathered)
    factor = head_dim ** -0.5 * LOG2E
    sub = 256
    n_sub = groups * chunk // sub

    def kernel(rank_ref, q_ref, *refs):
        kv_refs = refs[:n_chunk]
        o_ref, k_buf, v_buf, top_ref, total_ref, acc_ref, sems = refs[n_chunk:]
        g = pl.program_id(0)
        me = rank_ref[0]

        def copies(j, c):
            rows = pl.ds(pl.multiple_of(j * chunk, chunk), chunk)
            return (
                pltpu.make_async_copy(kv_refs[c].at[rows, pl.ds(pl.multiple_of(g * head_dim, head_dim), head_dim)], k_buf.at[c], sems.at[0, c]),
                pltpu.make_async_copy(kv_refs[c].at[rows, pl.ds(pl.multiple_of((nkv_heads + g) * head_dim, head_dim), head_dim)], v_buf.at[c], sems.at[1, c]),
            )

        def start(j, c):
            for copy in copies(j, c):
                copy.start()

        def wait(j, c):
            for copy in copies(j, c):
                copy.wait()

        def step(c, diagonal):
            for r in range(n_sub):
                head, part = divmod(r, chunk // sub)
                rows = slice(r * sub, (r + 1) * sub)
                q_rows = q_ref[part * sub:(part + 1) * sub, head * head_dim:(head + 1) * head_dim]
                s = dot_t(q_rows, k_buf[c])
                if diagonal:
                    row = lax.broadcasted_iota(jnp.int32, (sub, chunk), 0) + part * sub
                    col = lax.broadcasted_iota(jnp.int32, (sub, chunk), 1)
                    s = jnp.where(col <= row, s, NEG_BIG)
                old = top_ref[rows, 0:1]
                new = jnp.maximum(old, jnp.max(s, axis=1, keepdims=True))
                alpha = jnp.exp2((old - new) * factor)
                p = jnp.exp2((s - new) * factor)
                total_ref[rows, 0:1] = total_ref[rows, 0:1] * alpha + jnp.sum(p, axis=1, keepdims=True)
                acc_ref[rows, :] = acc_ref[rows, :] * alpha + jnp.dot(p.astype(BF16), v_buf[c], preferred_element_type=F32)
                top_ref[rows, 0:1] = new

        for c in range(n_chunk):
            start(0, c)
        top_ref[...] = jnp.full_like(top_ref, NEG_BIG)
        total_ref[...] = jnp.zeros_like(total_ref)
        acc_ref[...] = jnp.zeros_like(acc_ref)

        @pl.loop(0, me)
        def _(j):
            for c in range(n_chunk):
                wait(j, c)
                step(c, False)
                start(j + 1, c)

        for c in range(n_chunk):
            wait(me, c)
            if c < n_own:
                step(c, c == n_own - 1)
        for r in range(n_sub):
            head, part = divmod(r, chunk // sub)
            rows = slice(r * sub, (r + 1) * sub)
            o_ref[part * sub:(part + 1) * sub, head * head_dim:(head + 1) * head_dim] = (acc_ref[rows, :] / total_ref[rows, 0:1]).astype(BF16)

    return run_kernel(
        kernel, (q, *gathered),
        [pl.BlockSpec((chunk, groups * head_dim), lambda i, f: (0, i))] + [ANY] * n_chunk,
        sds((chunk, nq), BF16), pl.BlockSpec((chunk, groups * head_dim), lambda i, f: (0, i)), (nkv_heads,),
        scalars=(rank,), deps=deps,
        scratch=[pltpu.VMEM((n_chunk, chunk, head_dim), BF16), pltpu.VMEM((n_chunk, chunk, head_dim), BF16),
                 pltpu.VMEM((groups * chunk, 128), F32), pltpu.VMEM((groups * chunk, 128), F32),
                 pltpu.VMEM((groups * chunk, head_dim), F32), pltpu.SemaphoreType.DMA((2, n_chunk))],
        flops=4 * chunk * (2 * n_chunk * chunk) * nq, nbytes=16 * chunk * nq,
    )


def out_project(layer, tp_id, o_own, o_other, w_o, w_other, x, x_block, norm_gain, deps):
    chunk, k_own = o_own.shape
    width = w_o.shape[-1]
    bm = chunk // 2
    sub = 128

    def half(i, tp):
        return lax.rem(i + 1 + tp[0], 2)

    def kernel(tp, own_ref, oth_ref, w_own, w_oth, x_ref, ng, r_ref, m_ref):
        for part in range(bm // sub):
            rows = slice(part * sub, (part + 1) * sub)
            attn = jnp.dot(own_ref[rows, :], w_own[...], preferred_element_type=F32) + jnp.dot(oth_ref[rows, :], w_oth[...], preferred_element_type=F32)
            resid = (x_ref[rows, :].astype(F32) + rms_scale(attn, ng[1:2, :])).astype(BF16)
            r_ref[rows, :] = resid
            m_ref[rows, :] = rms_scale(resid.astype(F32), ng[2:3, :]).astype(BF16)

    return run_kernel(
        kernel, (o_own, o_other, w_o, w_other, x, norm_gain),
        [pl.BlockSpec((bm, k_own), lambda i, tp: (half(i, tp), 0)), pl.BlockSpec((bm, k_own), lambda i, tp: (half(i, tp), 0)),
         once((None, k_own, width), lambda i, tp: (layer, 0, 0)), once((k_own, width), lambda i, tp: (0, 0)),
         pl.BlockSpec((bm, width), lambda i, tp: (2 * x_block + half(i, tp), 0)),
         once((None,) + norm_gain.shape[1:], lambda i, tp: (layer, 0, 0))],
        (sds((chunk, width), BF16), sds((chunk, width), BF16)),
        [pl.BlockSpec((bm, width), lambda i, tp: (i, 0)), pl.BlockSpec((bm, width), lambda i, tp: (i, 0))],
        (2,), scalars=(tp_id,), deps=deps,
        flops=4 * chunk * k_own * width, nbytes=4 * k_own * width + 8 * chunk * width,
    )


def mlp_partial(layer, m, w_gate, w_up, w_down, deps):
    chunk, width = m.shape
    ff = w_gate.shape[-1]
    bf = 512
    bm = chunk // 2
    steps = ff // bf

    def kernel(m_ref, wg, wu, wd, send_ref, keep_ref):
        step = pl.program_id(0)
        for part, out_ref in ((0, send_ref), (1, keep_ref)):
            rows = m_ref[part * bm:(part + 1) * bm, :]
            gate = jnp.dot(rows, wg[...], preferred_element_type=F32)
            up = jnp.dot(rows, wu[...], preferred_element_type=F32)
            act = (jax.nn.gelu(gate, approximate=True) * up).astype(BF16)

            @pl.when(step == 0)
            def _():
                out_ref[...] = jnp.dot(act, wd[...], preferred_element_type=F32)

            @pl.when(step > 0)
            def _():
                out_ref[...] += jnp.dot(act, wd[...], preferred_element_type=F32)

    return run_kernel(
        kernel, (m, w_gate, w_up, w_down),
        [once((chunk, width), lambda i: (0, 0)),
         pl.BlockSpec((None, width, bf), lambda i: (layer, 0, i)), pl.BlockSpec((None, width, bf), lambda i: (layer, 0, i)),
         pl.BlockSpec((None, bf, width), lambda i: (layer, i, 0))],
        (sds((bm, width), F32), sds((bm, width), F32)),
        [pl.BlockSpec((bm, width), lambda i: (0, 0)), pl.BlockSpec((bm, width), lambda i: (0, 0))],
        (steps,), deps=deps, flops=6 * chunk * width * ff, nbytes=6 * width * ff + 6 * chunk * width,
    )


def finish_rows(layer, kept, received, r, norm_gain, deps):
    rows, width = kept.shape
    bm = 128
    skip = rows // bm

    def kernel(kept_ref, recv_ref, r_ref, ng, x_ref):
        x_ref[...] = (r_ref[...].astype(F32) + rms_scale(kept_ref[...] + recv_ref[...], ng[3:4, :])).astype(BF16)

    return run_kernel(
        kernel, (kept, received, r, norm_gain),
        [pl.BlockSpec((bm, width), lambda i: (i, 0)), pl.BlockSpec((bm, width), lambda i: (i, 0)),
         pl.BlockSpec((bm, width), lambda i: (skip + i, 0)), once((None,) + norm_gain.shape[1:], lambda i: (layer, 0, 0))],
        sds((rows, width), BF16), pl.BlockSpec((bm, width), lambda i: (i, 0)), (rows // bm,), deps=deps,
        flops=20 * rows * width, nbytes=12 * rows * width,
    )


def place_rows(tp_id, x_keep, x_other, row0, total_rows, target, deps):
    bm, width = x_keep.shape
    b0 = row0 // bm

    def half(i, tp):
        return lax.rem(i + tp[0], 2)

    def kernel(tp, keep_ref, other_ref, *refs):
        refs[-1][...] = jnp.where(pl.program_id(0) == 0, keep_ref[...], other_ref[...])

    specs = [once((bm, width), lambda i, tp: (0, 0)), once((bm, width), lambda i, tp: (0, 0))]
    args = [x_keep, x_other]
    aliases = None
    if target is not None:
        specs.append(ANY)
        args.append(target)
        aliases = {3: 0}
    return run_kernel(
        kernel, args, specs, sds((total_rows, width), BF16),
        pl.BlockSpec((bm, width), lambda i, tp: (b0 + half(i, tp), 0)), (2,), scalars=(tp_id,), deps=deps, aliases=aliases,
        flops=bm * width, nbytes=8 * bm * width,
    )


SEQUENCE = (
    ("swap", 0, 0), ("qkv", 0, 1), ("halo", 0, 0), ("qkv", 0, 0), ("attn", 0, 2), ("attn", 0, 3), ("attn", 0, 0), ("attn", 0, 1),
    ("wo", 0, 2), ("mlp", 0, 2), ("wo", 0, 3), ("mlp", 0, 3), ("wo", 0, 0), ("mlp", 0, 0), ("post", 0, 2),
    ("wo", 0, 1), ("mlp", 0, 1), ("post", 0, 3), ("post", 0, 0), ("cache", 0, 0), ("qkv", 1, 2), ("post", 0, 1), ("swap", 1, 0),
    ("qkv", 1, 3), ("qkv", 1, 0), ("qkv", 1, 1),
    ("attn", 1, 2), ("attn", 1, 3), ("wo", 1, 2), ("mlp", 1, 2), ("attn", 1, 0), ("wo", 1, 3), ("mlp", 1, 3), ("attn", 1, 1),
    ("cache", 1, 0), ("wo", 1, 0), ("mlp", 1, 0), ("post", 1, 2), ("wo", 1, 1), ("mlp", 1, 1), ("post", 1, 3), ("post", 1, 0),
    ("place", 1, 2), ("place", 1, 3), ("post", 1, 1), ("place", 1, 0), ("place", 1, 1),
)


def solution(mesh):
    cp_size = mesh.shape['cp']
    tp_size = mesh.shape['tp']
    assert tp_size == 2
    row_spec = P(('dp', 'cp'), None)
    col_spec = P(None, None, 'tp')
    row_w_spec = P(None, 'tp', None)
    cache_spec = P(None, ('dp', 'cp'), 'tp', None)
    swap = [(0, 1), (1, 0)]

    def device_fn(hidden, positions, w_q, w_k, w_v, w_o, w_gate, w_up, w_down, norm_gain, qk_gain):
        tok_rows, width = hidden.shape
        head_dim = qk_gain.shape[-1]
        half_dim = head_dim // 2
        kv_width = w_k.shape[-1]
        chunk = 512
        n_chunk = tok_rows // chunk
        high = tok_rows // 2
        tp_id = lax.axis_index('tp').astype(jnp.int32).reshape(1)
        cp_id = lax.axis_index('cp').astype(jnp.int32)
        rank = cp_id.reshape(1)
        first = (cp_id == 0).astype(jnp.int32).reshape(1)

        def exchange(value):
            return lax.ppermute(value, 'tp', swap)

        theta_col = jnp.array(THETAS, F32)[:, None]
        inv_freq = theta_col ** (-(jnp.arange(half_dim, dtype=F32) * 2.0) / head_dim)[None, :]
        base_pos = (positions[0] + 32 * jnp.arange(tok_rows // 32, dtype=jnp.int32)).astype(F32)
        base_ang = base_pos[None, :, None] * inv_freq[:, None, :]
        off_ang = jnp.arange(32, dtype=F32)[None, :, None] * inv_freq[:, None, :]
        tabs = (jnp.stack([jnp.cos(base_ang), jnp.sin(base_ang)], axis=1), jnp.stack([jnp.cos(off_ang), jnp.sin(off_ang)], axis=1))

        quarter = w_o.shape[1] // cp_size
        qkv_weights = (w_q, w_k, w_v, norm_gain, qk_gain)
        w_other, q_rot, kv_own, kv_all, x_mid = {}, {}, {}, {}, {}
        o_own, o_oth, r_rows, m_rows, kept, recv, x_keep, x_oth = {}, {}, {}, {}, {}, {}, {}, {}
        halo = None
        out = None
        caches = [jnp.zeros((2, tok_rows, kv_width // head_dim, head_dim), BF16) for _ in range(2)]
        deps = ()

        for kind, layer, c in SEQUENCE:
            if kind == "swap":
                piece = lax.dynamic_slice(w_o, (layer, cp_id * quarter, 0), (1, quarter, width))[0]
                if deps:
                    piece, _ = lax.optimization_barrier((piece, deps[0]))
                w_other[layer] = lax.all_gather(exchange(piece), 'cp', axis=0, tiled=True)
                continue
            if kind == "halo":
                halo = lax.ppermute(kv_own[0, 1], 'cp', [(i, i + 1) for i in range(cp_size - 1)])
                continue
            if kind == "cache":
                pieces = [(kv_own[0, b], b * high) for b in range(2)] if layer == 0 else [(kv_own[1, b], b * chunk) for b in range(n_chunk)]
                tied = lax.optimization_barrier(tuple(p for p, _ in pieces) + tuple(deps))[: len(pieces)]
                for which in range(2):
                    for piece, (_, row) in zip(tied, pieces):
                        part = piece[:, which * kv_width:(which + 1) * kv_width].reshape(1, piece.shape[0], kv_width // head_dim, head_dim)
                        caches[which] = lax.dynamic_update_slice(caches[which], part, (layer, row, 0, 0))
                deps = (*deps, *caches)
                continue
            if kind == "qkv" and layer == 0:
                q_rot[0, c], kv_own[0, c] = qkv_from_rows(0, hidden, c * high, high, qkv_weights, tabs, deps)
                result = q_rot[0, c]
            elif kind == "qkv":
                q_rot[1, c], kv_own[1, c], x_mid[c] = qkv_from_pieces(1, tp_id, x_keep[0, c], x_oth[0, c], c * chunk, qkv_weights, tabs, deps)
                kv_all[c] = lax.all_gather(kv_own[1, c], 'cp', axis=0, tiled=True)
                result = q_rot[1, c]
            elif kind == "attn" and layer == 0:
                per = high // chunk
                blocks = [(kv_own[0, b // per], b % per, False) if b >= 0 else (halo, b + per, True) for b in (c - 2, c - 1, c)]
                result = o_own[c] = local_attention(first, q_rot[0, c // per], c % per, blocks, head_dim, chunk, deps)
                o_oth[c] = exchange(result)
            elif kind == "attn":
                result = o_own[c] = global_attention(rank, q_rot[1, c], [kv_all[i] for i in range(n_chunk)], c + 1, head_dim, chunk, deps)
                o_oth[c] = exchange(result)
            elif kind == "wo":
                x, x_block = (hidden, c) if layer == 0 else (x_mid[c], 0)
                r_rows[c], m_rows[c] = out_project(layer, tp_id, o_own[c], o_oth[c], w_o, w_other[layer], x, x_block, norm_gain, deps)
                result = r_rows[c]
            elif kind == "mlp":
                send, kept[c] = mlp_partial(layer, m_rows[c], w_gate, w_up, w_down, deps)
                recv[c] = exchange(send)
                result = kept[c]
            elif kind == "post":
                result = x_keep[layer, c] = finish_rows(layer, kept[c], recv[c], r_rows[c], norm_gain, deps)
                x_oth[layer, c] = exchange(result)
            elif kind == "place":
                result = out = place_rows(tp_id, x_keep[1, c], x_oth[1, c], c * chunk, tok_rows, out, deps if out is None or deps[0] is not out else ())
            deps = (result,)
        return out, caches[0], caches[1]

    return jax.shard_map(
        device_fn,
        mesh=mesh,
        in_specs=(row_spec, P(('dp', 'cp')), col_spec, col_spec, col_spec, row_w_spec, col_spec, col_spec, row_w_spec, P(), P()),
        out_specs=(row_spec, cache_spec, cache_spec),
        check_vma=False,
    )
```

```python
import functools

import jax
import jax.numpy as jnp
from jax import lax
from jax.experimental import pallas as pl
from jax.experimental.pallas import tpu as pltpu
from jax.sharding import PartitionSpec as P


THETAS = (10000.0, 1000000.0)
EPS = 1e-6
NEG_BIG = -1e30
LOG2E = 1.4426950408889634
F32 = jnp.float32
BF16 = jnp.bfloat16
VMEM_LIMIT = 67043328
ANY = pl.BlockSpec(memory_space=pl.ANY)


def rms_scale(values, gain):
    mean_sq = jnp.mean(values * values, axis=-1, keepdims=True)
    return values * lax.rsqrt(mean_sq + EPS) * (1.0 + gain)


def once(shape, index_map):
    return pl.BlockSpec(shape, index_map, pipeline_mode=pl.Buffered(1))


def run_kernel(kernel, args, in_specs, out_shape, out_specs, grid, scalars=(), deps=(), scratch=(), flops=0, nbytes=0, aliases=None):
    n_scalar = len(scalars)
    n_in = len(args)
    n_dep = len(deps)

    def body(*refs):
        head = refs[: n_scalar + n_in]
        tail = refs[n_scalar + n_in + n_dep:]
        kernel(*head, *tail)

    return pl.pallas_call(
        body,
        out_shape=out_shape,
        grid_spec=pltpu.PrefetchScalarGridSpec(
            num_scalar_prefetch=n_scalar,
            grid=grid,
            in_specs=list(in_specs) + [ANY] * n_dep,
            out_specs=out_specs,
            scratch_shapes=list(scratch),
        ),
        compiler_params=pltpu.CompilerParams(vmem_limit_bytes=VMEM_LIMIT, dimension_semantics=("arbitrary",) * len(grid)),
        cost_estimate=pl.CostEstimate(flops=int(flops), bytes_accessed=int(nbytes), transcendentals=0),
        input_output_aliases=aliases or {},
    )(*scalars, *args, *deps)


def copy_in(src, dst, sem):
    return pltpu.make_async_copy(src, dst, sem)


def sds(shape, dtype):
    return jax.ShapeDtypeStruct(shape, dtype)


def project_rows(x_rows, w_q, w_k, w_v, gain, qk_gain, base_tab, off_tab, q_out, kv_out, k_cache, v_cache, head_dim):
    normed = rms_scale(x_rows.astype(F32), gain).astype(BF16)
    rows = x_rows.shape[0]
    half = head_dim // 2
    cos_off, sin_off = off_tab[0], off_tab[1]
    cosines, sines = [], []
    for g in range(rows // 32):
        cos_base, sin_base = base_tab[0, g:g + 1, :], base_tab[1, g:g + 1, :]
        cosines.append(cos_base * cos_off - sin_base * sin_off)
        sines.append(sin_base * cos_off + cos_base * sin_off)
    cosine = jnp.concatenate(cosines, axis=0)
    sine_val = jnp.concatenate(sines, axis=0)

    def rotate(proj, head_gain):
        normed_head = rms_scale(proj, head_gain)
        lower, upper = normed_head[:, :half], normed_head[:, half:]
        return jnp.concatenate([lower * cosine - upper * sine_val, upper * cosine + lower * sine_val], axis=1).astype(BF16)

    n_kv = w_k.shape[-1] // head_dim
    kv_width = n_kv * head_dim
    for h in range(n_kv):
        cols = slice(h * head_dim, (h + 1) * head_dim)
        proj = jnp.dot(normed, w_k[:, cols], preferred_element_type=F32)
        kv_out[:, cols] = rotate(proj, qk_gain[1:2, :])
    for h in range(n_kv):
        cols = slice(h * head_dim, (h + 1) * head_dim)
        kv_out[:, kv_width + h * head_dim:kv_width + (h + 1) * head_dim] = jnp.dot(normed, w_v[:, cols], preferred_element_type=F32).astype(BF16)
    for h in range(w_q.shape[-1] // head_dim):
        cols = slice(h * head_dim, (h + 1) * head_dim)
        proj = jnp.dot(normed, w_q[:, cols], preferred_element_type=F32)
        q_out[:, cols] = rotate(proj, qk_gain[0:1, :])
    k_cache[...] = kv_out[:, :kv_width].reshape(rows, n_kv, head_dim)
    v_cache[...] = kv_out[:, kv_width:].reshape(rows, n_kv, head_dim)


def project(layer, tp_id, x_parts, row0, rows, weights, tabs, caches, total_rows, deps):
    w_q, w_k, w_v, norm_gain, qk_gain = weights
    base_tab, off_tab = tabs
    head_dim = qk_gain.shape[-1]
    paired = isinstance(x_parts, tuple)
    width = w_q.shape[1]
    bm = rows // 2 if paired else 256
    b0 = row0 // bm
    n_alias = 0 if caches is None else 2

    def block(i, tp):
        return lax.rem(i + tp[0], 2) if paired else i

    def kernel(tp, *refs):
        x_refs, refs = refs[:1 + paired], refs[1 + paired:]
        wq, wk, wv, ng, qg, bt, ot = refs[:7]
        outs = refs[7 + n_alias:]
        if paired:
            x_rows = jnp.where(pl.program_id(0) == 0, x_refs[0][...], x_refs[1][...])
            outs[4][...] = x_rows
        else:
            x_rows = x_refs[0][...]
        project_rows(x_rows, wq, wk, wv, ng[0:1, :], qg, bt, ot, *outs[:4], head_dim)

    nq, nkv = w_q.shape[-1], 2 * w_k.shape[-1]
    cache_shape = (2, total_rows, nkv // 2 // head_dim, head_dim)
    if paired:
        x_specs = [once((bm, width), lambda i, tp: (0, 0))] * 2
    else:
        x_specs = [pl.BlockSpec((bm, width), lambda i, tp: (b0 + i, 0))]
    cache_spec = pl.BlockSpec((None, bm) + cache_shape[2:], lambda i, tp: (layer, b0 + block(i, tp), 0, 0))
    in_specs = x_specs + [
        once((None,) + w_q.shape[1:], lambda i, tp: (layer, 0, 0)),
        once((None,) + w_k.shape[1:], lambda i, tp: (layer, 0, 0)),
        once((None,) + w_v.shape[1:], lambda i, tp: (layer, 0, 0)),
        once((None,) + norm_gain.shape[1:], lambda i, tp: (layer, 0, 0)),
        once((None,) + qk_gain.shape[1:], lambda i, tp: (layer, 0, 0)),
        pl.BlockSpec((None, 2, bm // 32, head_dim // 2), lambda i, tp: (layer, 0, b0 + block(i, tp), 0)),
        once((None, 2, 32, head_dim // 2), lambda i, tp: (layer, 0, 0, 0)),
    ] + [ANY] * n_alias
    out_shape = [sds((rows, nq), BF16), sds((rows, nkv), BF16), sds(cache_shape, BF16), sds(cache_shape, BF16)]
    out_specs = [pl.BlockSpec((bm, nq), lambda i, tp: (block(i, tp), 0)), pl.BlockSpec((bm, nkv), lambda i, tp: (block(i, tp), 0)), cache_spec, cache_spec]
    if paired:
        out_shape.append(sds((rows, width), BF16))
        out_specs.append(pl.BlockSpec((bm, width), lambda i, tp: (block(i, tp), 0)))
    args = (x_parts if paired else (x_parts,)) + tuple(weights) + (base_tab, off_tab) + (() if caches is None else tuple(caches))
    first_alias = 1 + len(args) - n_alias
    aliases = {first_alias + i: 2 + i for i in range(n_alias)}
    return run_kernel(
        kernel, args, in_specs, tuple(out_shape), out_specs, (rows // bm,), scalars=(tp_id,), deps=deps, aliases=aliases,
        flops=2 * rows * width * (nq + nkv), nbytes=2 * width * (nq + nkv + 2 * rows),
    )


def dot_t(a, b):
    return lax.dot_general(a, b, (((1,), (1,)), ((), ())), preferred_element_type=F32)


def causal(s):
    return jnp.where(lax.broadcasted_iota(jnp.int32, s.shape, 1) <= lax.broadcasted_iota(jnp.int32, s.shape, 0), s, NEG_BIG)


def windowed(s):
    return jnp.where(lax.broadcasted_iota(jnp.int32, s.shape, 1) > lax.broadcasted_iota(jnp.int32, s.shape, 0), s, NEG_BIG)


def row_max(scores):
    widest = max(s.shape[1] for s in scores)
    full = [s for s in scores if s.shape[1] == widest]
    tops = [jnp.max(functools.reduce(jnp.maximum, full), axis=1, keepdims=True)]
    tops += [jnp.max(s, axis=1, keepdims=True) for s in scores if s.shape[1] != widest]
    return functools.reduce(jnp.maximum, tops)


def row_sum(probs):
    widest = max(p.shape[1] for p in probs)
    full = [p for p in probs if p.shape[1] == widest]
    sums = [jnp.sum(functools.reduce(jnp.add, full), axis=1, keepdims=True)]
    sums += [jnp.sum(p, axis=1, keepdims=True) for p in probs if p.shape[1] != widest]
    return functools.reduce(jnp.add, sums)


def weighted(probs, values):
    return functools.reduce(jnp.add, [jnp.dot(p.astype(BF16), v, preferred_element_type=F32) for p, v in zip(probs, values)])


def local_attention(first, q, q_row, kv_blocks, head_dim, chunk, deps):
    nq = q.shape[1]
    nkv_heads = kv_blocks[0][0].shape[1] // (2 * head_dim)
    groups = nq // head_dim // nkv_heads
    factor = head_dim ** -0.5 * LOG2E
    sub = 256
    q_block = q_row // chunk

    def kernel(first_ref, q_ref, ka, va, kb, vb, kc, vc, o_ref):
        key_refs, val_refs = (ka, kb, kc), (va, vb, vc)
        units = [(g, r) for g in range(groups) for r in range(chunk // sub)]

        def pieces(r):
            out = []
            for b in range(3):
                for p in range(chunk // sub):
                    if b == 1 or (b == 0 and p > r) or (b == 2 and p < r):
                        out.append((b, p * sub, None))
                    elif p == r:
                        out.append((b, p * sub, windowed if b == 0 else causal))
            return out

        def scores_of(unit):
            g, r = unit
            q_rows = q_ref[r * sub:(r + 1) * sub, g * head_dim:(g + 1) * head_dim]
            scores = []
            for b, key0, mask in pieces(r):
                s = dot_t(q_rows, key_refs[b][key0:key0 + sub, :])
                if mask is not None:
                    s = mask(s)
                if kv_blocks[b][2]:
                    s = jnp.where(first_ref[0] == 1, NEG_BIG, s)
                scores.append(s)
            return scores

        scores = scores_of(units[0])
        for at, (g, r) in enumerate(units):
            later = scores_of(units[at + 1]) if at + 1 < len(units) else None
            top = row_max(scores)
            probs = [jnp.exp2((s - top) * factor) for s in scores]
            out = weighted(probs, [val_refs[b][key0:key0 + sub, :] for b, key0, _ in pieces(r)])
            o_ref[r * sub:(r + 1) * sub, g * head_dim:(g + 1) * head_dim] = (out / row_sum(probs)).astype(BF16)
            scores = later

    specs = [pl.BlockSpec((chunk, groups * head_dim), lambda i, f: (q_block, i))]
    args = [q]
    for array, block, _ in kv_blocks:
        specs.append(pl.BlockSpec((chunk, head_dim), lambda i, f, block=block: (block, i)))
        specs.append(pl.BlockSpec((chunk, head_dim), lambda i, f, block=block: (block, nkv_heads + i)))
        args += [array, array]
    return run_kernel(
        kernel, args, specs, sds((chunk, nq), BF16),
        pl.BlockSpec((chunk, groups * head_dim), lambda i, f: (0, i)), (nkv_heads,),
        scalars=(first,), deps=deps, flops=4 * chunk * 3 * chunk * nq, nbytes=10 * chunk * nq,
    )


def global_attention(rank, q, own, sources, head_dim, deps):
    chunk, nq = q.shape
    kv_width = own[0][1].shape[1]
    nkv_heads = kv_width // (2 * head_dim)
    groups = nq // head_dim // nkv_heads
    factor = head_dim ** -0.5 * LOG2E
    sub = 256
    n_part = chunk // sub
    units = [(g, r) for g in range(groups) for r in range(n_part)]
    q_start = own[-1][0]
    own_rows = q_start + chunk
    src_rows = sum(a.shape[0] for _, a in sources[0])
    piece = 512
    n_own, n_src = len(own), len(sources[0])

    def kernel(rank_ref, q_ref, *refs):
        own_refs, refs = refs[:n_own], refs[n_own:]
        src_refs, refs = [refs[i * n_src:(i + 1) * n_src] for i in range(3)], refs[3 * n_src:]
        o_ref, own_buf, src_buf, top_ref, total_ref, acc_ref, own_sems, src_sems = refs
        me = rank_ref[0]

        def own_copies():
            return [copy_in(ref, own_buf.at[row:row + ref.shape[0]], own_sems.at[i]) for i, (ref, (row, _)) in enumerate(zip(own_refs, own))]

        def src_copies(which, slot):
            return [copy_in(ref, src_buf.at[slot, row:row + ref.shape[0]], src_sems.at[slot, i]) for i, (ref, (row, _)) in enumerate(zip(src_refs[which], sources[0]))]

        def start_source(j):
            which = j + jnp.where(me == 2, 1, 0)
            slot = lax.rem(j, 2)
            for w in range(3):
                @pl.when(which == w)
                def _():
                    for copy in src_copies(w, slot):
                        copy.start()

        for copy in own_copies():
            copy.start()

        @pl.when(me > 0)
        def _():
            start_source(0)

        for copy in own_copies():
            copy.wait()

        def unit_refs(h, unit):
            g, r = unit
            rows = slice((g * n_part + r) * sub, (g * n_part + r + 1) * sub)
            q_rows = q_ref[r * sub:(r + 1) * sub, pl.ds(pl.multiple_of((h * groups + g) * head_dim, head_dim), head_dim)]
            return rows, q_rows

        def key_cols(h):
            return pl.ds(pl.multiple_of(h * head_dim, head_dim), head_dim)

        def val_cols(h):
            return pl.ds(pl.multiple_of((nkv_heads + h) * head_dim, head_dim), head_dim)

        @pl.loop(0, nkv_heads)
        def _(h):
            def bounds(r):
                limit = q_start + r * sub
                return [(i, min(i + piece, limit)) for i in range(0, limit, piece)] + [(limit, limit + sub)]

            def scores_of(unit):
                _, q_rows = unit_refs(h, unit)
                scores = [dot_t(q_rows, own_buf[lo:hi, key_cols(h)]) for lo, hi in bounds(unit[1])]
                return scores[:-1] + [causal(scores[-1])]

            scores = scores_of(units[0])
            for at, unit in enumerate(units):
                later = scores_of(units[at + 1]) if at + 1 < len(units) else None
                rows, _ = unit_refs(h, unit)
                top = row_max(scores)
                probs = [jnp.exp2((s - top) * factor) for s in scores]
                top_ref[h, rows, 0:1] = top
                total_ref[h, rows, 0:1] = row_sum(probs)
                acc_ref[h, rows, :] = weighted(probs, [own_buf[lo:hi, val_cols(h)] for lo, hi in bounds(unit[1])])
                scores = later

        @pl.loop(0, me)
        def _(j):
            slot = lax.rem(j, 2)
            for copy in src_copies(0, slot):
                copy.wait()

            @pl.when(j + 1 < me)
            def _():
                start_source(j + 1)

            @pl.loop(0, nkv_heads)
            def _(h):
                bounds = [(i, min(i + piece, src_rows)) for i in range(0, src_rows, piece)]

                def scores_of(unit):
                    _, q_rows = unit_refs(h, unit)
                    return [dot_t(q_rows, src_buf[slot, lo:hi, key_cols(h)]) for lo, hi in bounds]

                scores = scores_of(units[0])
                for at, unit in enumerate(units):
                    later = scores_of(units[at + 1]) if at + 1 < len(units) else None
                    rows, _ = unit_refs(h, unit)
                    old = top_ref[h, rows, 0:1]
                    top = jnp.maximum(old, row_max(scores))
                    alpha = jnp.exp2((old - top) * factor)
                    probs = [jnp.exp2((s - top) * factor) for s in scores]
                    top_ref[h, rows, 0:1] = top
                    total_ref[h, rows, 0:1] = total_ref[h, rows, 0:1] * alpha + row_sum(probs)
                    acc_ref[h, rows, :] = acc_ref[h, rows, :] * alpha + weighted(probs, [src_buf[slot, lo:hi, val_cols(h)] for lo, hi in bounds])
                    scores = later

        for h in range(nkv_heads):
            for g, r in units:
                rows = slice((g * n_part + r) * sub, (g * n_part + r + 1) * sub)
                o_ref[r * sub:(r + 1) * sub, (h * groups + g) * head_dim:(h * groups + g + 1) * head_dim] = (acc_ref[h, rows, :] / total_ref[h, rows, 0:1]).astype(BF16)

    args = [q] + [a for _, a in own] + [a for s in sources for _, a in s]
    return run_kernel(
        kernel, args, [pl.BlockSpec((chunk, nq), lambda i, f: (0, 0))] + [ANY] * (len(args) - 1),
        sds((chunk, nq), BF16), pl.BlockSpec((chunk, nq), lambda i, f: (0, 0)), (1,),
        scalars=(rank,), deps=deps,
        scratch=[pltpu.VMEM((own_rows, kv_width), BF16), pltpu.VMEM((2, src_rows, kv_width), BF16),
                 pltpu.VMEM((nkv_heads, groups * chunk, 128), F32), pltpu.VMEM((nkv_heads, groups * chunk, 128), F32),
                 pltpu.VMEM((nkv_heads, groups * chunk, head_dim), F32),
                 pltpu.SemaphoreType.DMA((n_own,)), pltpu.SemaphoreType.DMA((2, n_src))],
        flops=4 * chunk * (2 * src_rows) * nq, nbytes=16 * chunk * nq,
    )


def out_mlp(layer, ids, o_own, o_other, w_o, w_pieces, x, x_row, norm_gain, w_gate, w_up, w_down, deps):
    chunk, k_own = o_own.shape
    width = w_o.shape[-1]
    ff = w_gate.shape[-1]
    bm = chunk // 2
    bf = 512
    steps = ff // bf
    bk = 512
    n_k = k_own // bk
    quarter = w_pieces[0].shape[0]
    sub = 128

    def kernel(ids_ref, own_ref, oth_ref, wo_ref, p0, p1, p2, p3, x_ref, wg_ref, wu_ref, wd_ref, ng,
               send_ref, keep_ref, r_ref, o_buf, w_buf, x_buf, r_buf, m_buf, act_buf, acc_ref, g_buf, u_buf, d_buf, o_sems, w_sems, x_sem, t_sems, out_sems):
        tp, cp = ids_ref[0], ids_ref[1]
        halves = (1 - tp, tp)

        def rows_of(i, base=0):
            return pl.ds(pl.multiple_of(base + halves[i] * bm, bm), bm)

        own_w = [copy_in(wo_ref.at[layer, b * bk:(b + 1) * bk], w_buf.at[b * bk:(b + 1) * bk], w_sems.at[b]) for b in range(n_k)]
        oth_w = [copy_in(ref, w_buf.at[pl.ds(pl.multiple_of(k_own + quarter * lax.bitwise_xor(cp, flip), quarter), quarter)], w_sems.at[n_k + i])
                 for i, (ref, flip) in enumerate(((p0, 0), (p1, 2), (p2, 1), (p3, 3)))]
        o_copies = [[copy_in(ref.at[rows_of(i)], o_buf.at[i * bm:(i + 1) * bm, part * k_own:(part + 1) * k_own], o_sems.at[part, i]) for i in range(2)]
                    for part, ref in enumerate((own_ref, oth_ref))]
        x_copies = [copy_in(x_ref.at[rows_of(i, x_row)], x_buf.at[i * bm:(i + 1) * bm], x_sem.at[i]) for i in range(2)]

        def tile_copies(t, slot):
            cols = pl.ds(pl.multiple_of(t * bf, bf), bf)
            return (copy_in(wg_ref.at[layer, :, cols], g_buf.at[slot], t_sems.at[0, slot]),
                    copy_in(wu_ref.at[layer, :, cols], u_buf.at[slot], t_sems.at[1, slot]))

        def down_copy(t, slot):
            return copy_in(wd_ref.at[layer, pl.ds(pl.multiple_of(t * bf, bf), bf)], d_buf.at[slot], t_sems.at[2, slot])

        for copy in (*o_copies[0], own_w[0], own_w[1], *o_copies[1], *oth_w, *x_copies, *tile_copies(0, 0), down_copy(0, 0)):
            copy.start()

        for copy in o_copies[0]:
            copy.wait()
        for b in range(n_k):
            own_w[b].wait()
            part = jnp.dot(o_buf[:, b * bk:(b + 1) * bk], w_buf[b * bk:(b + 1) * bk, :], preferred_element_type=F32)
            acc_ref[...] = part if b == 0 else acc_ref[...] + part
        for copy in (*o_copies[1], *oth_w, *x_copies):
            copy.wait()
        other = jnp.dot(o_buf[:, k_own:], w_buf[k_own:, :], preferred_element_type=F32)
        acc_ref[...] = acc_ref[...] + other
        for row in range(0, chunk, sub):
            rows = slice(row, row + sub)
            resid = (x_buf[rows, :].astype(F32) + rms_scale(acc_ref[rows, :], ng[1:2, :])).astype(BF16)
            if row >= bm:
                r_buf[row - bm:row - bm + sub, :] = resid
            m_buf[rows, :] = rms_scale(resid.astype(F32), ng[2:3, :]).astype(BF16)
        r_copy = copy_in(r_buf, r_ref, out_sems.at[2])
        r_copy.start()

        def up_gate(slot):
            gate = jnp.dot(m_buf[...], g_buf[slot], preferred_element_type=F32)
            up = jnp.dot(m_buf[...], u_buf[slot], preferred_element_type=F32)
            return gate, up

        def activate(gate, up, slot):
            act_buf[slot] = (jax.nn.gelu(gate, approximate=True) * up).astype(BF16)

        for copy in tile_copies(0, 0):
            copy.wait()
        for copy in tile_copies(1, 1):
            copy.start()
        activate(*up_gate(0), 0)
        acc_ref[...] = jnp.zeros_like(acc_ref)

        @pl.loop(1, steps)
        def _(t):
            slot = lax.rem(t, 2)
            old = 1 - slot
            for copy in tile_copies(t, slot):
                copy.wait()
            down_copy(t - 1, old).wait()
            down_copy(t, slot).start()

            @pl.when(t + 1 < steps)
            def _():
                for copy in tile_copies(t + 1, old):
                    copy.start()

            gate, up = up_gate(slot)
            acc_ref[...] += jnp.dot(act_buf[old], d_buf[old], preferred_element_type=F32)
            activate(gate, up, slot)

        last = (steps - 1) % 2
        down_copy(steps - 1, last).wait()
        outs = []
        for i, ref in enumerate((send_ref, keep_ref)):
            rows = slice(i * bm, (i + 1) * bm)
            acc_ref[rows, :] += jnp.dot(act_buf[last, rows, :], d_buf[last], preferred_element_type=F32)
            outs.append(copy_in(acc_ref.at[rows], ref, out_sems.at[i]))
            outs[-1].start()
        for copy in outs:
            copy.wait()
        r_copy.wait()

    args = (o_own, o_other, w_o, *w_pieces, x, w_gate, w_up, w_down, norm_gain)
    return run_kernel(
        kernel, args, [ANY] * (len(args) - 1) + [pl.BlockSpec((None,) + norm_gain.shape[1:], lambda i, s: (layer, 0, 0))],
        (sds((bm, width), F32), sds((bm, width), F32), sds((bm, width), BF16)), [ANY] * 3, (1,), scalars=(ids,), deps=deps,
        scratch=[pltpu.VMEM((chunk, 2 * k_own), BF16), pltpu.VMEM((2 * k_own, width), BF16), pltpu.VMEM((chunk, width), BF16),
                 pltpu.VMEM((bm, width), BF16), pltpu.VMEM((chunk, width), BF16), pltpu.VMEM((2, chunk, bf), BF16), pltpu.VMEM((chunk, width), F32),
                 pltpu.VMEM((2, width, bf), BF16), pltpu.VMEM((2, width, bf), BF16), pltpu.VMEM((2, bf, width), BF16),
                 pltpu.SemaphoreType.DMA((2, 2)), pltpu.SemaphoreType.DMA((n_k + 4,)), pltpu.SemaphoreType.DMA((2,)),
                 pltpu.SemaphoreType.DMA((3, 2)), pltpu.SemaphoreType.DMA((3,))],
        flops=4 * chunk * k_own * width + 6 * chunk * width * ff, nbytes=6 * width * ff + 4 * k_own * width + 20 * chunk * width,
    )


def finish_rows(layer, kept, received, r, norm_gain, deps):
    rows, width = kept.shape
    bm = 64

    def kernel(kept_ref, recv_ref, r_ref, ng, x_ref):
        x_ref[...] = (r_ref[...].astype(F32) + rms_scale(kept_ref[...] + recv_ref[...], ng[3:4, :])).astype(BF16)

    row_spec = pl.BlockSpec((bm, width), lambda i: (i, 0))
    return run_kernel(
        kernel, (kept, received, r, norm_gain),
        [row_spec, row_spec, row_spec, once((None,) + norm_gain.shape[1:], lambda i: (layer, 0, 0))],
        sds((rows, width), BF16), row_spec, (rows // bm,), deps=deps, flops=20 * rows * width, nbytes=12 * rows * width,
    )


def place_rows(tp_id, x_keep, x_other, row0, total_rows, target, deps):
    bm, width = x_keep.shape
    b0 = row0 // bm

    def half(i, tp):
        return lax.rem(i + tp[0], 2)

    def kernel(tp, keep_ref, other_ref, *refs):
        refs[-1][...] = jnp.where(pl.program_id(0) == 0, keep_ref[...], other_ref[...])

    specs = [once((bm, width), lambda i, tp: (0, 0)), once((bm, width), lambda i, tp: (0, 0))]
    args = [x_keep, x_other]
    aliases = None
    if target is not None:
        specs.append(ANY)
        args.append(target)
        aliases = {3: 0}
    return run_kernel(
        kernel, args, specs, sds((total_rows, width), BF16),
        pl.BlockSpec((bm, width), lambda i, tp: (b0 + half(i, tp), 0)), (2,), scalars=(tp_id,), deps=deps, aliases=aliases,
        flops=bm * width, nbytes=8 * bm * width,
    )


CHUNKS = ((0, 512), (512, 512), (1024, 512), (1536, 512))
SEQUENCE = (
    ("swap", 0, 0), ("qkv", 0, 1), ("halo", 0, 0), ("qkv", 0, 0), ("swapx", 0, 0), ("attn", 0, 2), ("attn", 0, 3), ("attn", 0, 0), ("attn", 0, 1),
    ("swapd", 0, 0), ("wm", 0, 2), ("wm", 0, 3), ("wm", 0, 0), ("post", 0, 2), ("wm", 0, 1), ("post", 0, 3), ("post", 0, 0),
    ("qkv", 1, 2), ("post", 0, 1), ("swap", 1, 0), ("qkv", 1, 3), ("fwd", 1, 2), ("qkv", 1, 0), ("fwd", 1, 3), ("qkv", 1, 1),
    ("fwd", 1, 0), ("swapx", 1, 0), ("fwd", 1, 1),
    ("attn", 1, 2), ("attn", 1, 3), ("swapd", 1, 0), ("wm", 1, 2), ("attn", 1, 0), ("wm", 1, 3), ("attn", 1, 1), ("wm", 1, 0), ("post", 1, 2),
    ("wm", 1, 1), ("post", 1, 3), ("post", 1, 0), ("place", 1, 2), ("place", 1, 3), ("post", 1, 1), ("place", 1, 0), ("place", 1, 1),
)


def solution(mesh):
    assert mesh.shape['cp'] == 4 and mesh.shape['tp'] == 2
    row_spec = P(('dp', 'cp'), None)
    col_spec = P(None, None, 'tp')
    row_w_spec = P(None, 'tp', None)
    cache_spec = P(None, ('dp', 'cp'), 'tp', None)
    swap_tp = [(0, 1), (1, 0)]
    swap_core = [(0, 1), (1, 0), (2, 3), (3, 2)]
    swap_chip = [(0, 2), (2, 0), (1, 3), (3, 1)]

    def device_fn(hidden, positions, w_q, w_k, w_v, w_o, w_gate, w_up, w_down, norm_gain, qk_gain):
        tok_rows, width = hidden.shape
        head_dim = qk_gain.shape[-1]
        half_dim = head_dim // 2
        high = tok_rows // 2
        tp_index = lax.axis_index('tp').astype(jnp.int32)
        cp_index = lax.axis_index('cp').astype(jnp.int32)
        tp_id, rank = tp_index.reshape(1), cp_index.reshape(1)
        ids = jnp.stack([tp_index, cp_index])
        first = (cp_index == 0).astype(jnp.int32).reshape(1)

        def permute(value, axis, pairs):
            return lax.ppermute(value, axis, pairs)

        def tied(value):
            return lax.optimization_barrier((value, deps[0]))[0] if deps else value

        theta_col = jnp.array(THETAS, F32)[:, None]
        inv_freq = theta_col ** (-(jnp.arange(half_dim, dtype=F32) * 2.0) / head_dim)[None, :]
        base_pos = (positions[0] + 32 * jnp.arange(tok_rows // 32, dtype=jnp.int32)).astype(F32)
        base_ang = base_pos[None, :, None] * inv_freq[:, None, :]
        off_ang = jnp.arange(32, dtype=F32)[None, :, None] * inv_freq[:, None, :]
        tabs = (jnp.stack([jnp.cos(base_ang), jnp.sin(base_ang)], axis=1), jnp.stack([jnp.cos(off_ang), jnp.sin(off_ang)], axis=1))

        quarter = w_o.shape[1] // 4
        weights = (w_q, w_k, w_v, norm_gain, qk_gain)
        w_pieces, q_rot, kv_own, kv_d, kv_x, kv_f, x_mid = {}, {}, {}, {}, {}, {}, {}
        o_own, o_oth, r_rows, kept, recv, x_keep, x_oth = {}, {}, {}, {}, {}, {}, {}
        halo = out = caches = None
        deps = ()

        for kind, layer, c in SEQUENCE:
            row, rows = (c * high, high) if kind == "qkv" and layer == 0 else CHUNKS[c]
            result = None
            if kind == "swap":
                piece = lax.dynamic_slice(w_o, (layer, cp_index * quarter, 0), (1, quarter, width))[0]
                w_pieces[layer] = [permute(tied(piece), 'tp', swap_tp)]
            elif kind == "swapx":
                w_pieces[layer].append(permute(tied(w_pieces[layer][0]), 'cp', swap_chip))
            elif kind == "swapd":
                w_pieces[layer] += [permute(tied(w_pieces[layer][0]), 'cp', swap_core), permute(tied(w_pieces[layer][1]), 'cp', swap_core)]
            elif kind == "halo":
                halo = permute(kv_own[0, 1], 'cp', [(i, i + 1) for i in range(3)])
            elif kind == "qkv" and layer == 0:
                q_rot[0, c], kv_own[0, c], *caches = project(0, tp_id, hidden, row, rows, weights, tabs, caches, tok_rows, deps)
                result = q_rot[0, c]
            elif kind == "qkv":
                q_rot[1, c], kv_own[1, c], *caches, x_mid[c] = project(1, tp_id, (x_keep[0, c], x_oth[0, c]), row, rows, weights, tabs, caches, tok_rows, deps)
                result = q_rot[1, c]
                kv_d[c] = permute(kv_own[1, c], 'cp', swap_core)
                kv_x[c] = permute(kv_own[1, c], 'cp', swap_chip)
            elif kind == "fwd":
                kv_f[c] = permute(tied(kv_x[c]), 'cp', swap_core)
            elif kind == "attn" and layer == 0:
                blocks = []
                for start in (row - 2 * rows, row - rows, row):
                    array = halo if start < 0 else kv_own[0, start // high]
                    blocks.append((array, start % high // rows, start < 0))
                result = o_own[c] = local_attention(first, q_rot[0, row // high], row % high, blocks, head_dim, rows, deps)
            elif kind == "attn":
                own = [(start, kv_own[1, i]) for i, (start, _) in enumerate(CHUNKS) if start <= row]
                sources = [[(CHUNKS[i][0], held[i]) for i in range(len(CHUNKS))] for held in (kv_d, kv_x, kv_f)]
                result = o_own[c] = global_attention(rank, q_rot[1, c], own, sources, head_dim, deps)
            elif kind == "wm":
                x, x_row = (hidden, row) if layer == 0 else (x_mid[c], 0)
                send, kept[c], r_rows[c] = out_mlp(layer, ids, o_own[c], o_oth[c], w_o, w_pieces[layer], x, x_row, norm_gain, w_gate, w_up, w_down, deps)
                recv[c] = permute(send, 'tp', swap_tp)
                result = kept[c]
            elif kind == "post":
                result = x_keep[layer, c] = finish_rows(layer, kept[c], recv[c], r_rows[c], norm_gain, deps)
                x_oth[layer, c] = permute(result, 'tp', swap_tp)
            elif kind == "place":
                result = out = place_rows(tp_id, x_keep[1, c], x_oth[1, c], row, tok_rows, out, deps if out is None or deps[0] is not out else ())
            if kind == "attn":
                o_oth[c] = permute(result, 'tp', swap_tp)
            if result is not None:
                deps = (result,)
        return out, caches[0], caches[1]

    return jax.shard_map(
        device_fn,
        mesh=mesh,
        in_specs=(row_spec, P(('dp', 'cp')), col_spec, col_spec, col_spec, row_w_spec, col_spec, col_spec, row_w_spec, P(), P()),
        out_specs=(row_spec, cache_spec, cache_spec),
        check_vma=False,
    )
```
